32 devices in a mesh: tile: 8 (over y, x, core), mode: 4 (over z).
Axes of the slice: x: 2, y: 2, z: 4, core: 2. Of those that a mesh axis runs over, the one named last changes fastest.
Arguments:
- object_tiles: float32 [8, 2, 2, 128, 128], P('tile'), may hold values from -1.5 to 1.5
- probe: float32 [16, 2, 128, 128], P('mode'), may hold values from -1 to 1
- propagator_phase: float32 [128, 128], replicated, may hold values from -3.140625 to 3.140625
- measured: float32 [32, 128, 128], P('tile'), may hold values from 0.25 to 2
- positions: int32 [32, 2], P('tile'), may hold values from 0 to 128, as said below
Outputs:
- updated_object: float32 [8, 2, 2, 128, 128], P('tile')
- intensity: float32 [32, 128, 128], P('tile')
The draws below stay inside these ranges and needn't reach their ends.
Inputs may be any that keep to these rules, and one draw needn't show every extreme that they name: `positions`: row and column of the top-left cell of a pattern's 128 x 128 window within its tile's extended region.
All inputs are finite; a program needn't handle non-finite values.
Results may differ from the reference program's by a relative error of at most 0.0003.
Values sent between devices are 32-bit elements; how exact they have to be, the bound alone decides.
No kernel may reach another device: no remote copies, remote signals or barrier semaphores. Data moves between devices by JAX's collectives and lax.ppermute only.
A program may use at most 64 MiB of HBM per device.

```python
import math
import jax
import jax.numpy as jnp
from jax import lax

K = 128
CORE = 128
HALO = 64
SLICES = 2
SCANS = 2
STEPS = 2
TILE_COLS = 8
MODES = 16
TILES = 8
PATTERNS = 32


def draw_positions(key, part):
    span_size = CORE + 2 * HALO - K + 1
    key_rows = jax.random.fold_in(key, 11)
    key_cols = jax.random.fold_in(key, 23)
    key_edge = jax.random.fold_in(key, 37)
    rows_drawn = jax.random.randint(key_rows, (PATTERNS,), 0, span_size)
    cols_drawn = jax.random.randint(key_cols, (PATTERNS,), 0, span_size)
    near_edge = jax.random.randint(key_edge, (PATTERNS,), 0, HALO // 2)
    pattern_index = jnp.arange(PATTERNS, dtype=jnp.int32)
    scan_index = pattern_index % SCANS
    cols_drawn = jnp.where(scan_index == 0, near_edge, cols_drawn)
    cols_drawn = jnp.where(scan_index == 1, span_size - 1 - near_edge, cols_drawn)
    return jnp.stack([rows_drawn, cols_drawn], axis=1).astype(jnp.int32)


def levels(rng, dims, split, smallest, largest):
    def one(dim, parts):
        heights = jax.random.uniform(jax.random.fold_in(jax.random.fold_in(rng, 6), dim), (parts,), jnp.float32, smallest / len(split), largest / len(split))
        return jnp.repeat(jnp.exp(heights), dims[dim] // parts).reshape((-1,) + (1,) * (len(dims) - dim - 1))

    factor_of = one(*split[0])
    for cut in split[1:]:
        factor_of = factor_of * one(*cut)
    return factor_of


def scatter_about(rng, shape, spread, most, shards=(), held_as=jnp.bfloat16):
    entries = spread * jax.random.normal(rng, shape, jnp.float32)
    if shards:
        entries = entries * levels(rng, shape, shards, -0.22, 0.18)
    return jnp.clip(entries, -most, most).astype(held_as)


def setup_inputs(seed: int = 0) -> dict:
    streams_of = jax.random.split(jax.random.key(seed), 6)
    object_tiles = scatter_about(streams_of[0], (TILES, SLICES, 2, CORE, CORE), 0.3, 1.5, ((0, 8),), jnp.float32)
    probe = scatter_about(streams_of[1], (MODES, 2, K, K), 0.18, 1.0, ((0, 4),), jnp.float32)
    propagator_phase = jnp.clip(jax.random.uniform(streams_of[2], (K, K), jnp.float32, -3.140625, 3.140625), -3.140625, 3.140625)
    measured = jnp.clip(0.25 + 1.75 * jax.random.uniform(streams_of[3], (PATTERNS, K, K), jnp.float32) ** levels(streams_of[3], (PATTERNS, K, K), ((0, 8),), -0.2, 0.2), 0.25, 2.0)
    positions = draw_positions(jax.random.fold_in(streams_of[5], 71), 0)
    return dict(object_tiles=object_tiles, probe=probe, propagator_phase=propagator_phase, measured=measured, positions=positions)


learning_rate = 0.5

def dft_tables(order_size):
    index = jnp.arange(order_size, dtype=jnp.int32)
    product = index[:, None] * index[None, :] % order_size
    angle = product.astype(jnp.float32) * (2.0 * math.pi / order_size)
    factor = 1.0 / math.sqrt(order_size)
    return (jnp.cos(angle) * factor, -jnp.sin(angle) * factor)

def product_left(matrix, operand):
    return jnp.einsum('jk,...kl->...jl', matrix, operand, precision=lax.Precision.HIGHEST)

def product_right(operand, matrix):
    return jnp.einsum('...jk,kl->...jl', operand, matrix, precision=lax.Precision.HIGHEST)

def transform(real_part, imag_part, cos_table, sin_table):
    left_real = product_left(cos_table, real_part) - product_left(sin_table, imag_part)
    left_imag = product_left(cos_table, imag_part) + product_left(sin_table, real_part)
    out_real = product_right(left_real, cos_table) - product_right(left_imag, sin_table)
    out_imag = product_right(left_imag, cos_table) + product_right(left_real, sin_table)
    return (out_real, out_imag)

def multislice(windows, probe, propagator_phase):
    order_size = probe.shape[-1]
    cos_table, sin_table = dft_tables(order_size)
    kernel_cos = jnp.cos(propagator_phase)
    kernel_sin = jnp.sin(propagator_phase)
    wave_real = probe[None, :, 0]
    wave_imag = probe[None, :, 1]
    layers = windows.shape[1]
    for layer_index in range(layers):
        trans_real = 1.0 + windows[:, None, layer_index, 0]
        trans_imag = windows[:, None, layer_index, 1]
        wave_real, wave_imag = (trans_real * wave_real - trans_imag * wave_imag, trans_real * wave_imag + trans_imag * wave_real)
        if layer_index + 1 < layers:
            spec_real, spec_imag = transform(wave_real, wave_imag, cos_table, sin_table)
            spec_real, spec_imag = (kernel_cos * spec_real - kernel_sin * spec_imag, kernel_cos * spec_imag + kernel_sin * spec_real)
            wave_real, wave_imag = transform(spec_real, spec_imag, cos_table, -sin_table)
    return transform(wave_real, wave_imag, cos_table, sin_table)

def windows_of(extended, positions, order_size):
    anchor = jnp.zeros((), jnp.int32)

    def single_window(position):
        starts = (anchor, anchor, position[0].astype(jnp.int32), position[1].astype(jnp.int32))
        return lax.dynamic_slice(extended, starts, (extended.shape[0], 2, order_size, order_size))
    return jax.vmap(single_window)(positions)

def neighbour_piece(tiles, tile_index, row_step, col_step):
    tile_count = tiles.shape[0]
    base = tile_index + row_step * TILE_COLS
    valid = jnp.logical_and(base >= 0, base < tile_count)
    target = jnp.mod(base + col_step, tile_count).astype(jnp.int32)
    piece = lax.dynamic_index_in_dim(tiles, target, 0, keepdims=False)
    core_size = tiles.shape[3]
    if row_step < 0:
        piece = piece[:, :, core_size - HALO:, :]
    elif row_step > 0:
        piece = piece[:, :, :HALO, :]
    if col_step < 0:
        piece = piece[:, :, :, core_size - HALO:]
    elif col_step > 0:
        piece = piece[:, :, :, :HALO]
    return piece * valid.astype(tiles.dtype)

def extend(tiles, tile_index):
    bands = []
    for row_step in (-1, 0, 1):
        band = [neighbour_piece(tiles, tile_index, row_step, col_step) for col_step in (-1, 0, 1)]
        bands.append(jnp.concatenate(band, axis=3))
    return jnp.concatenate(bands, axis=2)

def reference(object_tiles, probe, propagator_phase, measured, positions):
    tile_count = object_tiles.shape[0]
    tile_positions = positions.reshape(tile_count, STEPS, SCANS, 2)
    tile_measured = measured.reshape(tile_count, STEPS, SCANS, K, K)
    tiles = object_tiles
    outputs = []
    for iteration in range(STEPS):

        def tile_step(accumulated, inputs):
            tile_index, these_positions, these_measured = inputs

            def forward_tile(tiles_arg):
                return multislice(windows_of(extend(tiles_arg, tile_index), these_positions, K), probe, propagator_phase)
            (spec_real, spec_imag), pullback = jax.vjp(forward_tile, tiles)
            intensity = lax.optimization_barrier(jnp.sum(spec_real * spec_real + spec_imag * spec_imag, axis=1))
            residual = intensity - these_measured
            gradient, = pullback((2.0 * residual[:, None] * spec_real, 2.0 * residual[:, None] * spec_imag))
            return (accumulated + gradient, intensity)
        gradient, intensities = lax.scan(tile_step, jnp.zeros_like(tiles), (jnp.arange(tile_count, dtype=jnp.int32), tile_positions[:, iteration], tile_measured[:, iteration]))
        tiles = tiles - learning_rate * gradient
        outputs.append(intensities)
    stacked = jnp.stack(outputs, axis=0).transpose(1, 0, 2, 3, 4).reshape(tile_count * STEPS * SCANS, K, K)
    return (tiles, stacked)
```

```python
import math

import jax
import jax.numpy as jnp
import numpy as np
from jax import lax
from jax.experimental import pallas as pl
from jax.experimental.pallas import tpu as pltpu
from jax.sharding import PartitionSpec as P

HALO = 64
STEPS = 2
TILE_COLS = 8
SUB = 8

learning_rate = 0.5

f32 = jnp.float32
bf16 = jnp.bfloat16

VMEM = pl.BlockSpec(memory_space=pltpu.VMEM)
SMEM = pl.BlockSpec(memory_space=pltpu.SMEM)


def dft_matrix(order):
    index = np.arange(order)
    angle = (np.outer(index, index) % order) * (2.0 * math.pi / order)
    factor = 1.0 / math.sqrt(order)
    cos, sin = np.cos(angle) * factor, -np.sin(angle) * factor
    table = np.block([[cos, sin], [-sin, cos]])
    high = table.astype(bf16)
    low = (table - high.astype(np.float64)).astype(bf16)
    return np.stack([high, low])


def call(body, outs, args, scratch=(), mib=24):
    specs = [SMEM if a.dtype == jnp.int32 else VMEM for a in args]
    return pl.pallas_call(
        body,
        out_shape=[jax.ShapeDtypeStruct(s, f32) for s in outs],
        in_specs=specs,
        out_specs=[VMEM] * len(outs),
        scratch_shapes=list(scratch),
        compiler_params=pltpu.CompilerParams(vmem_limit_bytes=mib << 20),
    )(*args)


def halves(x):
    high = x.astype(bf16)
    return high, (x - high.astype(f32)).astype(bf16)


def product(x, high, low):
    xh, xl = halves(x)
    dot = lambda a, b: jnp.dot(a, b, preferred_element_type=f32)
    return dot(xh, high) + dot(xl, high) + dot(xh, low)


def flip(x, k):
    rows = []
    for i in range(x.shape[0] // k):
        part = x[i * k : (i + 1) * k]
        rows.append(jnp.concatenate([part[:, :k].T, part[:, k:].T], axis=1))
    return jnp.concatenate(rows, axis=0)


def dft(waves, high, low):
    k = waves[0].shape[0]
    x = jnp.concatenate(waves, axis=0)
    y = product(flip(product(x, high, low), k), high, low)
    return [y[i * k : (i + 1) * k] for i in range(len(waves))]


def pair(re, im):
    return jnp.concatenate([re, im], axis=1)


def window(plane, row, col, k):
    tall, width = k + SUB, plane.shape[1]
    base = pl.multiple_of(row - row % SUB, SUB)
    part = pltpu.roll(plane[pl.ds(base, tall), :], (width - col) % width, 1)[:, :k]
    return pltpu.roll(part, (tall - row % SUB) % tall, 0)[:k]


def add_window(ext, value, row, col):
    k, width = value.shape[0], ext.shape[1]
    wide = pltpu.roll(pair(value, jnp.zeros((k, width - k), f32)), col, 1)
    tall = jnp.concatenate([wide, jnp.zeros((SUB, width), f32)], axis=0)
    where = pl.ds(pl.multiple_of(row - row % SUB, SUB), k + SUB)
    ext[where, :] = ext[where, :] + pltpu.roll(tall, row % SUB, 0)


def forward_modes(windows, probes, cos_t, sin_t, table, u_outs, psi_outs, k):
    high, low = table[0], table[1]
    ar, ai, br, bi = [windows(p) for p in range(4)]
    ar, br = 1.0 + ar, 1.0 + br
    total = jnp.zeros((k, k), f32)
    for probe, u_out, psi_out in zip(probes, u_outs, psi_outs):
        count = probe.shape[0]
        waves = []
        for m in range(count):
            pr, pi = probe[m, 0], probe[m, 1]
            waves.append(pair(ar * pr - ai * pi, ar * pi + ai * pr))
        turned = []
        for s in dft(waves, high, low):
            sr, si = s[:, :k], s[:, k:]
            turned.append(pair(cos_t * sr - sin_t * si, -(cos_t * si + sin_t * sr)))
        waves = []
        for m, u in enumerate(dft(turned, high, low)):
            u_out[m] = u
            ur, ui = u[:, :k], u[:, k:]
            waves.append(pair(br * ur + bi * ui, bi * ur - br * ui))
        for m, psi in enumerate(dft(waves, high, low)):
            psi_out[m] = psi
            square = psi * psi
            total = total + (square[:, :k] + square[:, k:])
    return total.T


def first_forward(step_rows, rows):
    def body(z_ref, pos, *refs):
        if rows:
            ext_ref, probe, cos_t, sin_t, table = refs[:5]
            win, owned, part, u_out, psi_out, ext = refs[5:]
            ext[...] = ext_ref[...]
        else:
            tile, left, right, probe, cos_t, sin_t, table = refs[:7]
            win, owned, part, u_out, psi_out, ext = refs[7:]
            planes, core = tile.shape[0], tile.shape[1]
            ext[...] = jnp.zeros(ext.shape, f32)
            for p in range(planes):
                ext[p, HALO : HALO + core, :] = jnp.concatenate(
                    [left[p][:, core - HALO :], tile[p], right[p][:, :HALO]], axis=1
                )
        planes, k = win.shape[0], win.shape[1]
        z = z_ref[0]
        q = z % step_rows
        row, col = pos[q, 0], pos[q, 1]
        for p in range(planes):
            win[p] = window(ext.at[p], row, col, k)
        owned[...] = ext[z]
        part[...] = forward_modes(
            lambda p: win[p], [probe], cos_t[...], sin_t[...], table, [u_out], [psi_out], k
        )

    return body


def more_forward(win, probe, cos_t, sin_t, table, before, part, u_out, psi_out):
    k = win.shape[1]
    part[...] = before[...] + forward_modes(
        lambda p: win[p], [probe], cos_t[...], sin_t[...], table, [u_out], [psi_out], k
    )


def next_forward(count):
    def body(z_ref, *refs):
        pieces, refs = refs[:count], refs[count:]
        probe_a, probe_b, cos_t, sin_t, table, win, part, u_a, psi_a, u_b, psi_b = refs
        z = z_ref[0]
        k = win.shape[1]
        for j, piece in enumerate(pieces):
            win[(z + count - j) % count] = piece[...]
        part[...] = forward_modes(
            lambda p: win[p], [probe_a, probe_b], cos_t[...], sin_t[...], table,
            [u_a, u_b], [psi_a, psi_b], k,
        )

    return body


def backward(step, step_rows, parts, count):
    def body(z_ref, *refs):
        partials, refs = refs[:parts], refs[parts:]
        measured, win, probe_a, probe_b, u_a, psi_a, u_b, psi_b, cos_t, sin_t, table = refs[:11]
        intensity, sends, grads = refs[11], refs[12 : 12 + count], refs[12 + count]
        z = z_ref[0]
        k = win.shape[1]
        high, low = table[0], table[1]
        cos, sin = cos_t[...], sin_t[...]
        total = partials[0][...]
        for extra in partials[1:]:
            total = total + extra[...]
        intensity[...] = total
        twice = (2.0 * (total - measured[step * step_rows + z % step_rows])).T
        br, bi = 1.0 + win[2], win[3]
        zero = jnp.zeros((k, k), f32)
        g0r, g0i, g1r, g1i = zero, zero, zero, zero
        for probe, u_in, psi_in in ((probe_a, u_a, psi_a), (probe_b, u_b, psi_b)):
            modes = probe.shape[0]
            waves = []
            for m in range(modes):
                psi = psi_in[m]
                waves.append(pair(twice * psi[:, :k], -(twice * psi[:, k:])))
            turned = []
            for m, g in enumerate(dft(waves, high, low)):
                gr, gi = g[:, :k], -g[:, k:]
                u = u_in[m]
                ur, ui = u[:, :k], u[:, k:]
                g1r = g1r + (ur * gr - ui * gi)
                g1i = g1i + (ur * gi + ui * gr)
                turned.append(pair(br * gr + bi * gi, br * gi - bi * gr))
            waves = []
            for s in dft(turned, high, low):
                sr, si = s[:, :k], s[:, k:]
                waves.append(pair(cos * sr + sin * si, sin * sr - cos * si))
            for m, g in enumerate(dft(waves, high, low)):
                gr, gi = g[:, :k], -g[:, k:]
                pr, pi = probe[m, 0], probe[m, 1]
                g0r = g0r + (pr * gr + pi * gi)
                g0i = g0i + (pr * gi - pi * gr)
        grads[0], grads[1], grads[2], grads[3] = g0r, g0i, g1r, g1i
        for j in range(count):
            sends[j][...] = grads[(z + j) % count]

    return body


def scatter(step, step_rows, count, rows):
    def body(z_ref, pos, *refs):
        pieces, outs, ext = refs[:count], refs[count:-1], refs[-1]
        z = z_ref[0]
        q = z % step_rows
        width = ext.shape[1]
        ext[...] = jnp.zeros(ext.shape, f32)
        for i in range(step_rows):
            total = pieces[i][...]
            for j in range(i + step_rows, count, step_rows):
                total = total + pieces[j][...]
            which = step * step_rows + (q + step_rows - i) % step_rows
            add_window(ext, total, pos[which, 0], pos[which, 1])
        if rows:
            outs[0][...] = ext[...]
        else:
            half = width // 2
            core = outs[0].shape[0]
            outs[0][...] = ext[HALO : HALO + core, :half]
            outs[1][...] = ext[HALO : HALO + core, half:]

    return body


def updated_rows(left, right, from_left, from_right, owned):
    grad = pair(left[...] + from_left[...], right[...] + from_right[...])
    return owned[HALO : HALO + grad.shape[0], :] - learning_rate * grad


def next_windows(step, step_rows, source, z, pos, outs):
    q = z % step_rows
    k = outs[0].shape[0]
    for i, out in enumerate(outs):
        which = step * step_rows + (q + i) % step_rows
        row, col = pos[which, 0], pos[which, 1]
        out[...] = window(source, row, col, k)


def update(step, step_rows):
    def body(z_ref, pos, left, right, from_left, from_right, owned, fresh, *outs):
        fresh[...] = jnp.zeros(fresh.shape, f32)
        fresh[HALO : HALO + left.shape[0], :] = updated_rows(left, right, from_left, from_right, owned)
        next_windows(step, step_rows, fresh, z_ref[0], pos, outs)

    return body


def update_middle(left, right, from_left, from_right, owned, middle):
    middle[...] = updated_rows(left, right, from_left, from_right, owned)


def only_windows(step, step_rows):
    def body(z_ref, pos, owned, *outs):
        next_windows(step, step_rows, owned, z_ref[0], pos, outs)

    return body


def last_update(left, right, from_left, from_right, owned, core):
    middle = updated_rows(left, right, from_left, from_right, owned)
    core[...] = middle[:, HALO : middle.shape[1] - HALO]


def gather_planes(count):
    def body(z_ref, *refs):
        out = refs[count]
        for j in range(count):
            out[(z_ref[0] + count - j) % count] = refs[j][...]

    return body


def gather_intensities(step_rows):
    def body(z_ref, *refs):
        out = refs[-1]
        q = z_ref[0] % step_rows
        for i, ref in enumerate(refs[:-1]):
            step, j = divmod(i, step_rows)
            out[step * step_rows + (q + step_rows - j) % step_rows] = ref[...]

    return body


def ring(axis, steps):
    count = lax.axis_size(axis)
    return [(i, (i + steps) % count) for i in range(count)]


def shift(value, axis, steps):
    return lax.ppermute(value, axis, ring(axis, steps))


def from_behind(value, axis, steps):
    count = lax.axis_size(axis)
    first, last = (max(0, -steps), min(count, count - steps))
    return lax.ppermute(value, axis, [(source, source + steps) for source in range(first, last)])


def within(value, axis, group, steps):
    count = lax.axis_size(axis)
    pairs = [(i, i - i % group + (i % group + steps) % group) for i in range(count)]
    return lax.ppermute(value, axis, pairs)


def local(object_tiles, probe, propagator_phase, measured, positions):
    layers, core = object_tiles.shape[1], object_tiles.shape[3]
    count = layers * 2
    k = probe.shape[-1]
    modes = probe.shape[0]
    step_rows = positions.shape[0] // STEPS
    group = lax.axis_size("mode")
    assert layers == 2 and count == group and step_rows == 2 and core == 2 * HALO
    rows = lax.axis_size("tile") > TILE_COLS
    extent = core + 2 * HALO
    tall = (extent + SUB, extent)
    z = lax.axis_index("mode").astype(jnp.int32).reshape(1)
    planes = object_tiles.reshape(count, core, core)
    flat, wave = (k, k), (modes, k, 2 * k)

    other_probe = within(probe, "mode", step_rows, 1)
    from_left = shift(planes, "tile", 1)
    from_right = shift(planes, "tile", -1)
    cos_t, sin_t = jnp.cos(propagator_phase.T), jnp.sin(propagator_phase.T)
    table = jnp.asarray(dft_matrix(k))
    optics = (cos_t, sin_t, table)

    if rows:
        wide = jnp.concatenate(
            [from_left[:, :, core - HALO :], planes, from_right[:, :, :HALO]], axis=2
        )
        above = from_behind(wide[:, core - HALO :], "tile", TILE_COLS)
        below = from_behind(wide[:, :HALO], "tile", -TILE_COLS)
        slack = jnp.zeros((count, SUB, extent), f32)
        objects = (jnp.concatenate([above, wide, below, slack], axis=1),)
    else:
        objects = (planes, from_left, from_right)

    win, owned, part, u_a, psi_a = call(
        first_forward(step_rows, rows),
        [(count, k, k), tall, flat, wave, wave],
        (z, positions) + objects + (probe,) + optics,
        [pltpu.VMEM((count,) + tall, f32)],
    )
    part, u_b, psi_b = call(
        more_forward, [flat, wave, wave], (win, other_probe) + optics + (part,)
    )

    kept = []
    for step in range(STEPS):
        partials = [part] + [shift(part, "mode", j) for j in range(step_rows, group, step_rows)]
        out = call(
            backward(step, step_rows, len(partials), count),
            [flat] * (1 + count),
            (z,) + tuple(partials) + (measured, win, probe, other_probe, u_a, psi_a, u_b, psi_b) + optics,
            [pltpu.VMEM((count, k, k), f32)],
        )
        intensity, sends = out[0], out[1:]
        kept.append(intensity)
        kept.extend(within(intensity, "mode", step_rows, j) for j in range(1, step_rows))
        pieces = [sends[0]] + [shift(sends[j], "mode", j) for j in range(1, group)]
        half = (core, extent // 2)
        grads = call(
            scatter(step, step_rows, count, rows),
            [tall] if rows else [half, half],
            (z, positions) + tuple(pieces),
            [pltpu.VMEM(tall, f32)],
        )
        if rows:
            whole = grads[0]
            middle = whole[HALO : HALO + core]
            middle = middle.at[core - HALO :].add(from_behind(whole[:HALO], "tile", -TILE_COLS))
            middle = middle.at[:HALO].add(from_behind(whole[HALO + core : extent], "tile", TILE_COLS))
            grads = [middle[:, : extent // 2], middle[:, extent // 2 :]]
        left, right = grads
        sums = (left, right, shift(right, "tile", 1), shift(left, "tile", -1), owned)
        if step + 1 == STEPS:
            break
        if rows:
            (middle,) = call(update_middle, [(core, extent)], sums)
            above = from_behind(middle[core - HALO :], "tile", TILE_COLS)
            below = from_behind(middle[:HALO], "tile", -TILE_COLS)
            slack = jnp.zeros((SUB, extent), f32)
            owned = jnp.concatenate([above, middle, below, slack], axis=0)
            outs = call(only_windows(step + 1, step_rows), [flat] * step_rows, (z, positions, owned))
        else:
            out = call(
                update(step + 1, step_rows),
                [tall] + [flat] * step_rows,
                (z, positions) + sums,
            )
            owned, outs = out[0], out[1:]
        pieces = [outs[0]] + [shift(outs[j % step_rows], "mode", j) for j in range(1, group)]
        win, part, u_a, psi_a, u_b, psi_b = call(
            next_forward(count),
            [(count, k, k), flat, wave, wave, wave, wave],
            (z,) + tuple(pieces) + (probe, other_probe) + optics,
        )

    (plane,) = call(last_update, [(core, core)], sums)
    pieces = [plane] + [shift(plane, "mode", j) for j in range(1, group)]
    (updated,) = call(gather_planes(count), [(count, core, core)], (z,) + tuple(pieces))
    (intensities,) = call(gather_intensities(step_rows), [measured.shape], (z,) + tuple(kept))
    return (updated.reshape(object_tiles.shape), intensities)


def solution(mesh):
    return jax.shard_map(
        local,
        mesh=mesh,
        in_specs=(
            P("tile", None, None, None, None),
            P("mode", None, None, None),
            P(),
            P("tile", None, None),
            P("tile", None),
        ),
        out_specs=(P("tile", None, None, None, None), P("tile", None, None)),
        check_vma=False,
    )
```

```python
import math

import jax
import jax.numpy as jnp
import numpy as np
from jax import lax
from jax.experimental import pallas as pl
from jax.experimental.pallas import tpu as pltpu
from jax.sharding import PartitionSpec as P

HALO = 64
STEPS = 2
TILE_COLS = 8
SUB = 8
CHAIN = 2

learning_rate = 0.5

f32 = jnp.float32
bf16 = jnp.bfloat16

VMEM = pl.BlockSpec(memory_space=pltpu.VMEM)
SMEM = pl.BlockSpec(memory_space=pltpu.SMEM)


def dft_matrix(order):
    index = np.arange(order)
    angle = (np.outer(index, index) % order) * (2.0 * math.pi / order)
    factor = 1.0 / math.sqrt(order)
    cos, sin = np.cos(angle) * factor, -np.sin(angle) * factor
    table = np.block([[cos, sin], [-sin, cos]])
    high = table.astype(bf16)
    low = (table - high.astype(np.float64)).astype(bf16)
    return np.stack([high, low])


def call(body, outs, args, scratch=(), aliases=None, mib=24):
    specs = [SMEM if a.shape == (1,) else VMEM for a in args]
    return pl.pallas_call(
        body,
        out_shape=[jax.ShapeDtypeStruct(s, f32) for s in outs],
        in_specs=specs,
        out_specs=[VMEM] * len(outs),
        scratch_shapes=list(scratch),
        input_output_aliases=aliases or {},
        compiler_params=pltpu.CompilerParams(vmem_limit_bytes=mib << 20),
    )(*args)


def halves(x):
    high = x.astype(bf16)
    return high, (x - high.astype(f32)).astype(bf16)


def product(x, high, low):
    xh, xl = halves(x)
    dot = lambda a, b: jnp.dot(a, b, preferred_element_type=f32)
    return dot(xh, high) + dot(xl, high) + dot(xh, low)


def flip(x, k):
    rows = []
    for i in range(x.shape[0] // k):
        part = x[i * k : (i + 1) * k]
        rows.append(jnp.concatenate([part[:, :k].T, part[:, k:].T], axis=1))
    return jnp.concatenate(rows, axis=0)


def dft(waves, high, low):
    k = waves[0].shape[0]
    chains = [jnp.concatenate(waves[i : i + CHAIN], axis=0) for i in range(0, len(waves), CHAIN)]
    chains = [product(x, high, low) for x in chains]
    chains = [flip(x, k) for x in chains]
    chains = [product(x, high, low) for x in chains]
    return [y[i : i + k] for y in chains for i in range(0, y.shape[0], k)]


def pair(re, im):
    return jnp.concatenate([re, im], axis=1)


def window(plane, row, col, k):
    tall, width = k + SUB, plane.shape[1]
    base = pl.multiple_of(row - row % SUB, SUB)
    part = pltpu.roll(plane[pl.ds(base, tall), :], (width - col) % width, 1)[:, :k]
    return pltpu.roll(part, (tall - row % SUB) % tall, 0)[:k]


def add_window(ext, value, row, col):
    k, width = value.shape[0], ext.shape[1]
    wide = pltpu.roll(pair(value, jnp.zeros((k, width - k), f32)), col, 1)
    tall = jnp.concatenate([wide, jnp.zeros((SUB, width), f32)], axis=0)
    where = pl.ds(pl.multiple_of(row - row % SUB, SUB), k + SUB)
    ext[where, :] = ext[where, :] + pltpu.roll(tall, row % SUB, 0)


def spot(pos, which):
    value = pos[...].astype(f32)
    mine = lax.broadcasted_iota(jnp.int32, value.shape, 0) == which
    first = lax.broadcasted_iota(jnp.int32, value.shape, 1) == 0
    row = jnp.sum(jnp.where(mine & first, value, 0.0)).astype(jnp.int32)
    col = jnp.sum(jnp.where(mine & ~first, value, 0.0)).astype(jnp.int32)
    return row, col


def forward_modes(win, probes, cos_t, sin_t, table, u_out, psi_out, first, last):
    k = win.shape[1]
    high, low = table[0], table[1]
    cos, sin = cos_t[...], sin_t[...]
    ar, ai, br, bi = 1.0 + win[0], win[1], 1.0 + win[2], win[3]
    waves = []
    for m in range(first, last):
        pr, pi = probes[m, 0], probes[m, 1]
        waves.append(pair(ar * pr - ai * pi, ar * pi + ai * pr))
    turned = []
    for s in dft(waves, high, low):
        sr, si = s[:, :k], s[:, k:]
        turned.append(pair(cos * sr - sin * si, -(cos * si + sin * sr)))
    waves = []
    for m, u in enumerate(dft(turned, high, low), first):
        u_out[m] = u
        ur, ui = u[:, :k], u[:, k:]
        waves.append(pair(br * ur + bi * ui, bi * ur - br * ui))
    total = jnp.zeros((k, k), f32)
    for m, psi in enumerate(dft(waves, high, low), first):
        psi_out[m] = psi
        square = psi * psi
        total = total + (square[:, :k] + square[:, k:])
    return total.T


def pack(tile, to_left, to_right, copy):
    core = tile.shape[1]
    for p in range(0, tile.shape[0], 2):
        to_left[p // 2] = pair(tile[p][:, :HALO], tile[p + 1][:, :HALO])
        to_right[p // 2] = pair(tile[p][:, core - HALO :], tile[p + 1][:, core - HALO :])
    copy[...] = tile[...]


def hold(probe, probes):
    probes[0 : probe.shape[0]] = probe[...]


def first_forward(step_rows, rows):
    def body(index, pos, *refs):
        z = index[0]
        if rows:
            ext_ref, probes, cos_t, sin_t, table = refs[:5]
            win, owned, part, u_out, psi_out, ext = refs[5:]
            ext[...] = ext_ref[...]
        else:
            tile, from_left, from_right, probes, cos_t, sin_t, table = refs[:7]
            win, owned, part, u_out, psi_out, ext = refs[7:]
            planes, core = tile.shape[0], tile.shape[1]
            ext[...] = jnp.zeros(ext.shape, f32)
            for p in range(planes):
                at = slice(p % 2 * HALO, (p % 2 + 1) * HALO)
                ext[p, HALO : HALO + core, :] = jnp.concatenate(
                    [from_left[p // 2][:, at], tile[p], from_right[p // 2][:, at]], axis=1
                )
        planes, k = win.shape[0], win.shape[1]
        q = z % step_rows
        row, col = spot(pos, q)
        for p in range(planes):
            win[p] = window(ext.at[p], row, col, k)
        owned[...] = ext[z]
        half = probes.shape[0] // step_rows
        part[...] = forward_modes(win, probes, cos_t, sin_t, table, u_out, psi_out, 0, half)

    return body


def more_forward(win, probe, cos_t, sin_t, table, before, p_in, u_in, psi_in, part, probes, u_out, psi_out):
    first, last = probes.shape[0] - probe.shape[0], probes.shape[0]
    probes[first:last] = probe[...]
    part[...] = before[...] + forward_modes(
        win, probes, cos_t, sin_t, table, u_out, psi_out, first, last
    )


def next_forward(count):
    def body(index, *refs):
        pieces, refs = refs[:count], refs[count:]
        probes, cos_t, sin_t, table, win, part, u_out, psi_out = refs
        z = index[0]
        for j, piece in enumerate(pieces):
            win[z ^ j] = piece[...]
        part[...] = forward_modes(
            win, probes, cos_t, sin_t, table, u_out, psi_out, 0, probes.shape[0]
        )

    return body


def backward(step, step_rows, parts, count):
    def body(index, *refs):
        partials, refs = refs[:parts], refs[parts:]
        measured, win, probes, u_in, psi_in, cos_t, sin_t, table = refs[:8]
        sends, grads = refs[8 : 8 + count], refs[8 + count]
        z = index[0]
        k = win.shape[1]
        high, low = table[0], table[1]
        cos, sin = cos_t[...], sin_t[...]
        total = partials[0][...]
        for extra in partials[1:]:
            total = total + extra[...]
        sends[1][1] = total
        twice = (2.0 * (total - measured[step * step_rows + z % step_rows])).T
        br, bi = 1.0 + win[2], win[3]
        zero = jnp.zeros((k, k), f32)
        waves = []
        for m in range(probes.shape[0]):
            psi = psi_in[m]
            waves.append(pair(twice * psi[:, :k], -(twice * psi[:, k:])))
        turned = []
        sum_r, sum_i = zero, zero
        for m, g in enumerate(dft(waves, high, low)):
            gr, gi = g[:, :k], -g[:, k:]
            u = u_in[m]
            ur, ui = u[:, :k], u[:, k:]
            sum_r = sum_r + (ur * gr - ui * gi)
            sum_i = sum_i + (ur * gi + ui * gr)
            turned.append(pair(br * gr + bi * gi, br * gi - bi * gr))
        grads[2], grads[3] = sum_r, sum_i
        waves = []
        for s in dft(turned, high, low):
            sr, si = s[:, :k], s[:, k:]
            waves.append(pair(cos * sr + sin * si, sin * sr - cos * si))
        sum_r, sum_i = zero, zero
        for m, g in enumerate(dft(waves, high, low)):
            gr, gi = g[:, :k], -g[:, k:]
            pr, pi = probes[m, 0], probes[m, 1]
            sum_r = sum_r + (pr * gr + pi * gi)
            sum_i = sum_i + (pr * gi - pi * gr)
        grads[0], grads[1] = sum_r, sum_i
        for j in range(count):
            if j == 1:
                sends[j][0] = grads[z ^ j]
            else:
                sends[j][...] = grads[z ^ j]

    return body


def scatter(step, step_rows, count, rows):
    def body(index, pos, *refs):
        pieces, outs, ext = refs[:count], refs[count:-1], refs[-1]
        z = index[0]
        q = z % step_rows
        width = ext.shape[1]
        ext[...] = jnp.zeros(ext.shape, f32)
        values = [piece[0] if j == 1 else piece[...] for j, piece in enumerate(pieces)]
        for i in range(step_rows):
            total = values[i]
            for j in range(i + step_rows, count, step_rows):
                total = total + values[j]
            which = step * step_rows + (q ^ i)
            add_window(ext, total, *spot(pos, which))
        if rows:
            outs[0][...] = ext[...]
        else:
            half = width // 2
            core = outs[0].shape[0]
            middle = ext[HALO : HALO + core, :]
            outs[0][...], outs[1][...] = middle[:, :half], middle[:, half:]

    return body


def updated_rows(left, right, from_left, from_right, owned):
    grad = pair(left[...] + from_left[...], right[...] + from_right[...])
    return owned[HALO : HALO + grad.shape[0], :] - learning_rate * grad


def next_windows(step, step_rows, source, z, pos, outs):
    q = z % step_rows
    k = outs[0].shape[0]
    for i, out in enumerate(outs):
        which = step * step_rows + (q ^ i)
        out[...] = window(source, *spot(pos, which), k)


def update(step, step_rows):
    def body(index, pos, left, right, from_left, from_right, owned, fresh, *outs):
        z = index[0]
        fresh[...] = jnp.zeros(fresh.shape, f32)
        fresh[HALO : HALO + left.shape[0], :] = updated_rows(left, right, from_left, from_right, owned)
        next_windows(step, step_rows, fresh, z, pos, outs)

    return body


def update_middle(left, right, from_left, from_right, owned, middle):
    middle[...] = updated_rows(left, right, from_left, from_right, owned)


def only_windows(step, step_rows):
    def body(index, pos, owned, *outs):
        next_windows(step, step_rows, owned, index[0], pos, outs)

    return body


def last_update(left, right, from_left, from_right, owned, core):
    middle = updated_rows(left, right, from_left, from_right, owned)
    core[...] = middle[:, HALO : middle.shape[1] - HALO]


def gather_planes(count):
    def body(index, *refs):
        out = refs[count]
        for j in range(count):
            out[index[0] ^ j] = refs[j][...]

    return body


def gather_intensities(step_rows):
    def body(index, *refs):
        out = refs[-1]
        q = index[0] % step_rows
        for i, ref in enumerate(refs[:-1]):
            step, j = divmod(i, step_rows)
            out[step * step_rows + (q ^ j)] = ref[1]

    return body


def across(value, axis, bits):
    return lax.ppermute(value, axis, [(i, i ^ bits) for i in range(lax.axis_size(axis))])


def around(value, steps):
    count = lax.axis_size("tile")
    return lax.ppermute(value, "tile", [(i, (i + steps) % count) for i in range(count)])


def from_behind(value, axis, steps):
    count = lax.axis_size(axis)
    first, last = (max(0, -steps), min(count, count - steps))
    return lax.ppermute(value, axis, [(source, source + steps) for source in range(first, last)])


def local(object_tiles, probe, propagator_phase, measured, positions):
    layers, core = object_tiles.shape[1], object_tiles.shape[3]
    count = layers * 2
    k = probe.shape[-1]
    step_rows = positions.shape[0] // STEPS
    modes = probe.shape[0] * step_rows
    group, tiles = lax.axis_size("mode"), lax.axis_size("tile")
    assert layers == 2 and count == group and step_rows == 2 and core == 2 * HALO
    rows = tiles > TILE_COLS
    extent = core + 2 * HALO
    tall = (extent + SUB, extent)
    index = lax.axis_index("mode").astype(jnp.int32).reshape(1)
    planes = object_tiles.reshape(count, core, core)
    flat, wave, held = (k, k), (modes, k, 2 * k), (modes,) + probe.shape[1:]

    other_probe = across(probe, "mode", 1)
    packed = (count // 2, core, 2 * HALO)
    to_left, to_right, planes = call(pack, [packed, packed, planes.shape], (planes,))
    from_right, from_left = around(to_left, -1), around(to_right, 1)
    cos_t, sin_t = jnp.cos(propagator_phase.T), jnp.sin(propagator_phase.T)
    optics = (cos_t, sin_t, jnp.asarray(dft_matrix(k)))
    (probes,) = call(hold, [held], (probe,))

    if rows:

        def unpacked(value):
            return value.reshape(-1, core, 2, HALO).transpose(0, 2, 1, 3).reshape(count, core, HALO)

        wide = jnp.concatenate([unpacked(from_left), planes, unpacked(from_right)], axis=2)
        above = from_behind(wide[:, core - HALO :], "tile", TILE_COLS)
        below = from_behind(wide[:, :HALO], "tile", -TILE_COLS)
        slack = jnp.zeros((count, SUB, extent), f32)
        objects = (jnp.concatenate([above, wide, below, slack], axis=1),)
    else:
        objects = (planes, from_left, from_right)

    win, owned, part, u, psi = call(
        first_forward(step_rows, rows),
        [(count, k, k), tall, flat, wave, wave],
        (index, positions) + objects + (probes,) + optics,
        [pltpu.VMEM((count,) + tall, f32)],
    )
    part, probes, u, psi = call(
        more_forward,
        [flat, held, wave, wave],
        (win, other_probe) + optics + (part, probes, u, psi),
        aliases={6: 1, 7: 2, 8: 3},
    )

    kept = []
    for step in range(STEPS):
        partials = [part] + [across(part, "mode", j) for j in range(step_rows, group, step_rows)]
        sends = call(
            backward(step, step_rows, len(partials), count),
            [flat, (2,) + flat] + [flat] * (count - 2),
            (index,) + tuple(partials) + (measured, win, probes, u, psi) + optics,
            [pltpu.VMEM((count, k, k), f32)],
        )
        pieces = [sends[0]] + [across(sends[j], "mode", j) for j in range(1, group)]
        kept += [sends[1], pieces[1]]
        half = (core, extent // 2)
        grads = call(
            scatter(step, step_rows, count, rows),
            [tall] if rows else [half, half],
            (index, positions) + tuple(pieces),
            [pltpu.VMEM(tall, f32)],
        )
        if rows:
            whole = grads[0]
            middle = whole[HALO : HALO + core]
            middle = middle.at[core - HALO :].add(from_behind(whole[:HALO], "tile", -TILE_COLS))
            middle = middle.at[:HALO].add(from_behind(whole[HALO + core : extent], "tile", TILE_COLS))
            grads = (middle[:, : extent // 2], middle[:, extent // 2 :])
        left, right = grads
        sums = (left, right, around(right, 1), around(left, -1), owned)
        if step + 1 == STEPS:
            break
        if rows:
            (middle,) = call(update_middle, [(core, extent)], sums)
            above = from_behind(middle[core - HALO :], "tile", TILE_COLS)
            below = from_behind(middle[:HALO], "tile", -TILE_COLS)
            slack = jnp.zeros((SUB, extent), f32)
            owned = jnp.concatenate([above, middle, below, slack], axis=0)
            outs = call(only_windows(step + 1, step_rows), [flat] * step_rows, (index, positions, owned))
        else:
            out = call(
                update(step + 1, step_rows),
                [tall] + [flat] * step_rows,
                (index, positions) + sums,
            )
            owned, outs = out[0], out[1:]
        pieces = [outs[0]] + [across(outs[j % step_rows], "mode", j) for j in range(1, group)]
        win, part, u, psi = call(
            next_forward(count),
            [(count, k, k), flat, wave, wave],
            (index,) + tuple(pieces) + (probes,) + optics,
        )

    (plane,) = call(last_update, [(core, core)], sums)
    pieces = [plane] + [across(plane, "mode", j) for j in range(1, group)]
    (updated,) = call(gather_planes(count), [(count, core, core)], (index,) + tuple(pieces))
    (intensities,) = call(gather_intensities(step_rows), [measured.shape], (index,) + tuple(kept))
    return (updated.reshape(object_tiles.shape), intensities)


def solution(mesh):
    return jax.shard_map(
        local,
        mesh=mesh,
        in_specs=(
            P("tile", None, None, None, None),
            P("mode", None, None, None),
            P(),
            P("tile", None, None),
            P("tile", None),
        ),
        out_specs=(P("tile", None, None, None, None), P("tile", None, None)),
        check_vma=False,
    )
```

```python
import math

import jax
import jax.numpy as jnp
import numpy as np
from jax import lax
from jax.experimental import pallas as pl
from jax.experimental.pallas import tpu as pltpu
from jax.sharding import PartitionSpec as P

HALO = 64
STEPS = 2
TILE_COLS = 8
SUB = 8

learning_rate = 0.5

f32 = jnp.float32
bf16 = jnp.bfloat16

VMEM = pl.BlockSpec(memory_space=pltpu.VMEM)
SMEM = pl.BlockSpec(memory_space=pltpu.SMEM)


def dft_matrix(order):
    index = np.arange(order)
    angle = (np.outer(index, index) % order) * (2.0 * math.pi / order)
    factor = 1.0 / math.sqrt(order)
    cos, sin = np.cos(angle) * factor, -np.sin(angle) * factor
    table = np.block([[cos, sin], [-sin, cos]])
    high = table.astype(bf16)
    low = (table - high.astype(np.float64)).astype(bf16)
    return np.stack([high, low])


def call(body, outs, args, scratch=(), aliases=None, mib=24):
    specs = [SMEM if a.shape == (1,) else VMEM for a in args]
    return pl.pallas_call(
        body,
        out_shape=[jax.ShapeDtypeStruct(s, f32) for s in outs],
        in_specs=specs,
        out_specs=[VMEM] * len(outs),
        scratch_shapes=list(scratch),
        input_output_aliases=aliases or {},
        compiler_params=pltpu.CompilerParams(vmem_limit_bytes=mib << 20),
    )(*args)


def halves(x):
    high = x.astype(bf16)
    return high, (x - high.astype(f32)).astype(bf16)


def product(x, high, low):
    xh, xl = halves(x)
    dot = lambda a, b: jnp.dot(a, b, preferred_element_type=f32)
    return dot(xh, high) + dot(xl, high) + dot(xh, low)


def flip(x, k):
    rows = []
    for i in range(x.shape[0] // k):
        part = x[i * k : (i + 1) * k]
        rows.append(jnp.concatenate([part[:, :k].T, part[:, k:].T], axis=1))
    return jnp.concatenate(rows, axis=0)


def dft(waves, high, low):
    k, size = waves[0].shape[0], max(1, len(waves) // 4)
    chains = [jnp.concatenate(waves[i : i + size], axis=0) for i in range(0, len(waves), size)]
    chains = [product(x, high, low) for x in chains]
    chains = [flip(x, k) for x in chains]
    chains = [product(x, high, low) for x in chains]
    return [y[i : i + k] for y in chains for i in range(0, y.shape[0], k)]


def pair(re, im):
    return jnp.concatenate([re, im], axis=1)


def window(plane, row, col, k):
    tall, width = k + SUB, plane.shape[1]
    base = pl.multiple_of(row - row % SUB, SUB)
    part = pltpu.roll(plane[pl.ds(base, tall), :], (width - col) % width, 1)[:, :k]
    return pltpu.roll(part, (tall - row % SUB) % tall, 0)[:k]


def add_window(ext, value, row, col):
    k, width = value.shape[0], ext.shape[1]
    wide = pltpu.roll(pair(value, jnp.zeros((k, width - k), f32)), col, 1)
    tall = jnp.concatenate([wide, jnp.zeros((SUB, width), f32)], axis=0)
    where = pl.ds(pl.multiple_of(row - row % SUB, SUB), k + SUB)
    ext[where, :] = ext[where, :] + pltpu.roll(tall, row % SUB, 0)


def spot(pos, which):
    value = pos[...].astype(f32)
    mine = lax.broadcasted_iota(jnp.int32, value.shape, 0) == which
    first = lax.broadcasted_iota(jnp.int32, value.shape, 1) == 0
    row = jnp.sum(jnp.where(mine & first, value, 0.0)).astype(jnp.int32)
    col = jnp.sum(jnp.where(mine & ~first, value, 0.0)).astype(jnp.int32)
    return row, col


def forward_modes(win, probes, cos_t, sin_t, table, u_out, psi_out, first, last):
    k = win.shape[1]
    high, low = table[0], table[1]
    cos, sin = cos_t[...], sin_t[...]
    ar, ai, br, bi = 1.0 + win[0], win[1], 1.0 + win[2], win[3]
    waves = []
    for m in range(first, last):
        pr, pi = probes[m, 0], probes[m, 1]
        waves.append(pair(ar * pr - ai * pi, ar * pi + ai * pr))
    turned = []
    for s in dft(waves, high, low):
        sr, si = s[:, :k], s[:, k:]
        turned.append(pair(cos * sr - sin * si, -(cos * si + sin * sr)))
    waves = []
    for m, u in enumerate(dft(turned, high, low), first):
        u_out[m] = u
        ur, ui = u[:, :k], u[:, k:]
        waves.append(pair(br * ur + bi * ui, bi * ur - br * ui))
    total = jnp.zeros((k, k), f32)
    for m, psi in enumerate(dft(waves, high, low), first):
        psi_out[m] = psi
        square = psi * psi
        total = total + (square[:, :k] + square[:, k:])
    return total.T


def pack(tile, to_left, to_right, copy):
    core = tile.shape[1]
    for p in range(0, tile.shape[0], 2):
        to_left[p // 2] = pair(tile[p][:, :HALO], tile[p + 1][:, :HALO])
        to_right[p // 2] = pair(tile[p][:, core - HALO :], tile[p + 1][:, core - HALO :])
    copy[...] = tile[...]


def hold(probe, probes):
    probes[0 : probe.shape[0]] = probe[...]


def first_forward(step_rows, rows):
    def body(index, pos, *refs):
        z = index[0]
        if rows:
            ext_ref, probes, cos_t, sin_t, table = refs[:5]
            win, owned, part, u_out, psi_out, ext = refs[5:]
            ext[...] = ext_ref[...]
        else:
            tile, from_left, from_right, probes, cos_t, sin_t, table = refs[:7]
            win, owned, part, u_out, psi_out, ext = refs[7:]
            planes, core = tile.shape[0], tile.shape[1]
            ext[...] = jnp.zeros(ext.shape, f32)
            for p in range(planes):
                at = slice(p % 2 * HALO, (p % 2 + 1) * HALO)
                ext[p, HALO : HALO + core, :] = jnp.concatenate(
                    [from_left[p // 2][:, at], tile[p], from_right[p // 2][:, at]], axis=1
                )
        planes, k = win.shape[0], win.shape[1]
        q = z % step_rows
        row, col = spot(pos, q)
        for p in range(planes):
            win[p] = window(ext.at[p], row, col, k)
        owned[...] = ext[z]
        half = probes.shape[0] // step_rows
        part[...] = forward_modes(win, probes, cos_t, sin_t, table, u_out, psi_out, 0, half)

    return body


def more_forward(win, probe, cos_t, sin_t, table, before, p_in, u_in, psi_in, part, probes, u_out, psi_out):
    first, last = probes.shape[0] - probe.shape[0], probes.shape[0]
    probes[first:last] = probe[...]
    part[...] = before[...] + forward_modes(
        win, probes, cos_t, sin_t, table, u_out, psi_out, first, last
    )


def next_forward(count):
    def body(index, *refs):
        pieces, refs = refs[:count], refs[count:]
        probes, cos_t, sin_t, table, win, part, u_out, psi_out = refs
        z = index[0]
        for j, piece in enumerate(pieces):
            win[z ^ j] = piece[...]
        part[...] = forward_modes(
            win, probes, cos_t, sin_t, table, u_out, psi_out, 0, probes.shape[0]
        )

    return body


def backward(step, step_rows, parts, count):
    def body(index, *refs):
        partials, refs = refs[:parts], refs[parts:]
        measured, win, probes, u_in, psi_in, cos_t, sin_t, table = refs[:8]
        sends, grads = refs[8 : 8 + count], refs[8 + count]
        z = index[0]
        k = win.shape[1]
        high, low = table[0], table[1]
        cos, sin = cos_t[...], sin_t[...]
        total = partials[0][...]
        for extra in partials[1:]:
            total = total + extra[...]
        sends[1][1] = total
        twice = (2.0 * (total - measured[step * step_rows + z % step_rows])).T
        br, bi = 1.0 + win[2], win[3]
        zero = jnp.zeros((k, k), f32)
        waves = []
        for m in range(probes.shape[0]):
            psi = psi_in[m]
            waves.append(pair(twice * psi[:, :k], -(twice * psi[:, k:])))
        turned = []
        sum_r, sum_i = zero, zero
        for m, g in enumerate(dft(waves, high, low)):
            gr, gi = g[:, :k], -g[:, k:]
            u = u_in[m]
            ur, ui = u[:, :k], u[:, k:]
            sum_r = sum_r + (ur * gr - ui * gi)
            sum_i = sum_i + (ur * gi + ui * gr)
            turned.append(pair(br * gr + bi * gi, br * gi - bi * gr))
        grads[2], grads[3] = sum_r, sum_i
        waves = []
        for s in dft(turned, high, low):
            sr, si = s[:, :k], s[:, k:]
            waves.append(pair(cos * sr + sin * si, sin * sr - cos * si))
        sum_r, sum_i = zero, zero
        for m, g in enumerate(dft(waves, high, low)):
            gr, gi = g[:, :k], -g[:, k:]
            pr, pi = probes[m, 0], probes[m, 1]
            sum_r = sum_r + (pr * gr + pi * gi)
            sum_i = sum_i + (pr * gi - pi * gr)
        grads[0], grads[1] = sum_r, sum_i
        for j in range(count):
            if j == 1:
                sends[j][0] = grads[z ^ j]
            else:
                sends[j][...] = grads[z ^ j]

    return body


def scatter(step, step_rows, count, rows):
    def body(index, pos, *refs):
        pieces, outs, ext = refs[:count], refs[count:-1], refs[-1]
        z = index[0]
        q = z % step_rows
        width = ext.shape[1]
        ext[...] = jnp.zeros(ext.shape, f32)
        values = [piece[0] if j == 1 else piece[...] for j, piece in enumerate(pieces)]
        for i in range(step_rows):
            total = values[i]
            for j in range(i + step_rows, count, step_rows):
                total = total + values[j]
            which = step * step_rows + (q ^ i)
            add_window(ext, total, *spot(pos, which))
        if rows:
            outs[0][...] = ext[...]
        else:
            half = width // 2
            core = outs[0].shape[0]
            middle = ext[HALO : HALO + core, :]
            outs[0][...], outs[1][...] = middle[:, :half], middle[:, half:]

    return body


def updated_rows(left, right, from_left, from_right, owned):
    grad = pair(left[...] + from_left[...], right[...] + from_right[...])
    return owned[HALO : HALO + grad.shape[0], :] - learning_rate * grad


def next_windows(step, step_rows, source, z, pos, outs):
    q = z % step_rows
    k = outs[0].shape[0]
    for i, out in enumerate(outs):
        which = step * step_rows + (q ^ i)
        out[...] = window(source, *spot(pos, which), k)


def update(step, step_rows):
    def body(index, pos, left, right, from_left, from_right, owned, fresh, *outs):
        z = index[0]
        fresh[...] = jnp.zeros(fresh.shape, f32)
        fresh[HALO : HALO + left.shape[0], :] = updated_rows(left, right, from_left, from_right, owned)
        next_windows(step, step_rows, fresh, z, pos, outs)

    return body


def update_middle(left, right, from_left, from_right, owned, middle):
    middle[...] = updated_rows(left, right, from_left, from_right, owned)


def only_windows(step, step_rows):
    def body(index, pos, owned, *outs):
        next_windows(step, step_rows, owned, index[0], pos, outs)

    return body


def last_update(left, right, from_left, from_right, owned, core):
    middle = updated_rows(left, right, from_left, from_right, owned)
    core[...] = middle[:, HALO : middle.shape[1] - HALO]


def gather_planes(count):
    def body(index, *refs):
        out = refs[count]
        for j in range(count):
            out[index[0] ^ j] = refs[j][...]

    return body


def gather_intensities(step_rows):
    def body(index, *refs):
        out = refs[-1]
        q = index[0] % step_rows
        for i, ref in enumerate(refs[:-1]):
            step, j = divmod(i, step_rows)
            out[step * step_rows + (q ^ j)] = ref[1]

    return body


def across(value, axis, bits):
    return lax.ppermute(value, axis, [(i, i ^ bits) for i in range(lax.axis_size(axis))])


def around(value, steps):
    count = lax.axis_size("tile")
    return lax.ppermute(value, "tile", [(i, (i + steps) % count) for i in range(count)])


def from_behind(value, axis, steps):
    count = lax.axis_size(axis)
    first, last = (max(0, -steps), min(count, count - steps))
    return lax.ppermute(value, axis, [(source, source + steps) for source in range(first, last)])


def local(object_tiles, probe, propagator_phase, measured, positions):
    layers, core = object_tiles.shape[1], object_tiles.shape[3]
    count = layers * 2
    k = probe.shape[-1]
    step_rows = positions.shape[0] // STEPS
    modes = probe.shape[0] * step_rows
    group, tiles = lax.axis_size("mode"), lax.axis_size("tile")
    assert layers == 2 and count == group and step_rows == 2 and core == 2 * HALO
    rows = tiles > TILE_COLS
    extent = core + 2 * HALO
    tall = (extent + SUB, extent)
    index = lax.axis_index("mode").astype(jnp.int32).reshape(1)
    planes = object_tiles.reshape(count, core, core)
    flat, wave, held = (k, k), (modes, k, 2 * k), (modes,) + probe.shape[1:]

    other_probe = across(probe, "mode", 1)
    packed = (count // 2, core, 2 * HALO)
    to_left, to_right, planes = call(pack, [packed, packed, planes.shape], (planes,))
    from_right, from_left = around(to_left, -1), around(to_right, 1)
    cos_t, sin_t = jnp.cos(propagator_phase.T), jnp.sin(propagator_phase.T)
    optics = (cos_t, sin_t, jnp.asarray(dft_matrix(k)))
    (probes,) = call(hold, [held], (probe,))

    if rows:

        def unpacked(value):
            return value.reshape(-1, core, 2, HALO).transpose(0, 2, 1, 3).reshape(count, core, HALO)

        wide = jnp.concatenate([unpacked(from_left), planes, unpacked(from_right)], axis=2)
        above = from_behind(wide[:, core - HALO :], "tile", TILE_COLS)
        below = from_behind(wide[:, :HALO], "tile", -TILE_COLS)
        slack = jnp.zeros((count, SUB, extent), f32)
        objects = (jnp.concatenate([above, wide, below, slack], axis=1),)
    else:
        objects = (planes, from_left, from_right)

    win, owned, part, u, psi = call(
        first_forward(step_rows, rows),
        [(count, k, k), tall, flat, wave, wave],
        (index, positions) + objects + (probes,) + optics,
        [pltpu.VMEM((count,) + tall, f32)],
    )
    part, probes, u, psi = call(
        more_forward,
        [flat, held, wave, wave],
        (win, other_probe) + optics + (part, probes, u, psi),
        aliases={6: 1, 7: 2, 8: 3},
    )

    kept = []
    for step in range(STEPS):
        partials = [part] + [across(part, "mode", j) for j in range(step_rows, group, step_rows)]
        sends = call(
            backward(step, step_rows, len(partials), count),
            [flat, (2,) + flat] + [flat] * (count - 2),
            (index,) + tuple(partials) + (measured, win, probes, u, psi) + optics,
            [pltpu.VMEM((count, k, k), f32)],
        )
        pieces = [sends[0]] + [across(sends[j], "mode", j) for j in range(1, group)]
        kept += [sends[1], pieces[1]]
        half = (core, extent // 2)
        grads = call(
            scatter(step, step_rows, count, rows),
            [tall] if rows else [half, half],
            (index, positions) + tuple(pieces),
            [pltpu.VMEM(tall, f32)],
        )
        if rows:
            whole = grads[0]
            middle = whole[HALO : HALO + core]
            middle = middle.at[core - HALO :].add(from_behind(whole[:HALO], "tile", -TILE_COLS))
            middle = middle.at[:HALO].add(from_behind(whole[HALO + core : extent], "tile", TILE_COLS))
            grads = (middle[:, : extent // 2], middle[:, extent // 2 :])
        left, right = grads
        sums = (left, right, around(right, 1), around(left, -1), owned)
        if step + 1 == STEPS:
            break
        if rows:
            (middle,) = call(update_middle, [(core, extent)], sums)
            above = from_behind(middle[core - HALO :], "tile", TILE_COLS)
            below = from_behind(middle[:HALO], "tile", -TILE_COLS)
            slack = jnp.zeros((SUB, extent), f32)
            owned = jnp.concatenate([above, middle, below, slack], axis=0)
            outs = call(only_windows(step + 1, step_rows), [flat] * step_rows, (index, positions, owned))
        else:
            out = call(
                update(step + 1, step_rows),
                [tall] + [flat] * step_rows,
                (index, positions) + sums,
            )
            owned, outs = out[0], out[1:]
        pieces = [outs[0]] + [across(outs[j % step_rows], "mode", j) for j in range(1, group)]
        win, part, u, psi = call(
            next_forward(count),
            [(count, k, k), flat, wave, wave],
            (index,) + tuple(pieces) + (probes,) + optics,
        )

    (plane,) = call(last_update, [(core, core)], sums)
    pieces = [plane] + [across(plane, "mode", j) for j in range(1, group)]
    (updated,) = call(gather_planes(count), [(count, core, core)], (index,) + tuple(pieces))
    (intensities,) = call(gather_intensities(step_rows), [measured.shape], (index,) + tuple(kept))
    return (updated.reshape(object_tiles.shape), intensities)


def solution(mesh):
    return jax.shard_map(
        local,
        mesh=mesh,
        in_specs=(
            P("tile", None, None, None, None),
            P("mode", None, None, None),
            P(),
            P("tile", None, None),
            P("tile", None),
        ),
        out_specs=(P("tile", None, None, None, None), P("tile", None, None)),
        check_vma=False,
    )
```

```python
import math

import jax
import jax.numpy as jnp
import numpy as np
from jax import lax
from jax.experimental import pallas as pl
from jax.experimental.pallas import tpu as pltpu
from jax.sharding import PartitionSpec as P


HALO = 64
STEPS = 2
TILE_COLS = 8
SUB = 8

learning_rate = 0.5

f32 = jnp.float32
bf16 = jnp.bfloat16

VMEM = pl.BlockSpec(memory_space=pltpu.VMEM)
SMEM = pl.BlockSpec(memory_space=pltpu.SMEM)


def dft_matrix(order):
    index = np.arange(order)
    angle = (np.outer(index, index) % order) * (2.0 * math.pi / order)
    factor = 1.0 / math.sqrt(order)
    cos, sin = np.cos(angle) * factor, -np.sin(angle) * factor
    table = np.block([[cos, sin], [-sin, cos]])
    high = table.astype(bf16)
    low = (table - high.astype(np.float64)).astype(bf16)
    return np.stack([high, low])


def call(body, outs, args, scratch=(), aliases=None, mib=24):
    specs = [SMEM if a.shape == (1,) else VMEM for a in args]
    return pl.pallas_call(
        body,
        out_shape=[jax.ShapeDtypeStruct(s, f32) for s in outs],
        in_specs=specs,
        out_specs=[VMEM] * len(outs),
        scratch_shapes=list(scratch),
        input_output_aliases=aliases or {},
        compiler_params=pltpu.CompilerParams(vmem_limit_bytes=mib << 20),
    )(*args)


def halves(x):
    high = x.astype(bf16)
    return high, (x - high.astype(f32)).astype(bf16)


def product(x, high, low):
    xh, xl = halves(x)
    dot = lambda a, b: jnp.dot(a, b, preferred_element_type=f32)
    return dot(xh, high) + dot(xl, high) + dot(xh, low)


def flip(x, k):
    rows = []
    for i in range(x.shape[0] // k):
        part = x[i * k : (i + 1) * k]
        rows.append(jnp.concatenate([part[:, :k].T, part[:, k:].T], axis=1))
    return jnp.concatenate(rows, axis=0)


def dft(waves, high, low):
    k, size = waves[0].shape[0], max(1, len(waves) // 4)
    chains = [jnp.concatenate(waves[i : i + size], axis=0) for i in range(0, len(waves), size)]
    chains = [product(x, high, low) for x in chains]
    chains = [flip(x, k) for x in chains]
    chains = [product(x, high, low) for x in chains]
    return [y[i : i + k] for y in chains for i in range(0, y.shape[0], k)]


def pair(re, im):
    return jnp.concatenate([re, im], axis=1)


def window(plane, row, col, k):
    tall, width = k + SUB, plane.shape[1]
    base = pl.multiple_of(row - row % SUB, SUB)
    part = pltpu.roll(plane[pl.ds(base, tall), :], (width - col) % width, 1)[:, :k]
    return pltpu.roll(part, (tall - row % SUB) % tall, 0)[:k]


def add_window(ext, value, row, col):
    k, width = value.shape[0], ext.shape[1]
    wide = pltpu.roll(pair(value, jnp.zeros((k, width - k), f32)), col, 1)
    tall = jnp.concatenate([wide, jnp.zeros((SUB, width), f32)], axis=0)
    where = pl.ds(pl.multiple_of(row - row % SUB, SUB), k + SUB)
    ext[where, :] = ext[where, :] + pltpu.roll(tall, row % SUB, 0)


def spot(pos, which):
    value = pos[...].astype(f32)
    mine = lax.broadcasted_iota(jnp.int32, value.shape, 0) == which
    first = lax.broadcasted_iota(jnp.int32, value.shape, 1) == 0
    row = jnp.sum(jnp.where(mine & first, value, 0.0)).astype(jnp.int32)
    col = jnp.sum(jnp.where(mine & ~first, value, 0.0)).astype(jnp.int32)
    return row, col


def place(index, group):
    return index[0] % group, (index[0] // group) % 2


def forward_modes(win, probes, cos_t, sin_t, table, u_out, psi_out, first, last):
    k = win.shape[1]
    high, low = table[0], table[1]
    cos, sin = cos_t[...], sin_t[...]
    ar, ai, br, bi = 1.0 + win[0], win[1], 1.0 + win[2], win[3]
    waves = []
    for m in range(first, last):
        pr, pi = probes[m, 0], probes[m, 1]
        waves.append(pair(ar * pr - ai * pi, ar * pi + ai * pr))
    turned = []
    for s in dft(waves, high, low):
        sr, si = s[:, :k], s[:, k:]
        turned.append(pair(cos * sr - sin * si, -(cos * si + sin * sr)))
    waves = []
    for m, u in enumerate(dft(turned, high, low), first):
        u_out[m] = u
        ur, ui = u[:, :k], u[:, k:]
        waves.append(pair(br * ur + bi * ui, bi * ur - br * ui))
    total = jnp.zeros((k, k), f32)
    for m, psi in enumerate(dft(waves, high, low), first):
        psi_out[m] = psi
        square = psi * psi
        total = total + (square[:, :k] + square[:, k:])
    return total.T


def pack(group):
    def body(index, tile, out_a, out_b, copy):
        odd = place(index, group)[1] == 1
        core = tile.shape[1]
        for p in range(0, tile.shape[0], 2):
            left = pair(tile[p][:, :HALO], tile[p + 1][:, :HALO])
            right = pair(tile[p][:, core - HALO :], tile[p + 1][:, core - HALO :])
            out_a[p // 2] = jnp.where(odd, left, right)
            out_b[p // 2] = jnp.where(odd, right, left)
        copy[...] = tile[...]

    return body


def hold(probe, probes):
    probes[0 : probe.shape[0]] = probe[...]


def first_forward(step_rows, group, rows):
    def body(index, pos, *refs):
        z, parity = place(index, group)
        if rows:
            ext_ref, probes, cos_t, sin_t, table = refs[:5]
            win, owned, part, u_out, psi_out, ext = refs[5:]
            ext[...] = ext_ref[...]
        else:
            tile, from_a, from_b, probes, cos_t, sin_t, table = refs[:7]
            win, owned, part, u_out, psi_out, ext = refs[7:]
            planes, core = tile.shape[0], tile.shape[1]
            ext[...] = jnp.zeros(ext.shape, f32)
            for p in range(planes):
                at = slice(p % 2 * HALO, (p % 2 + 1) * HALO)
                left = jnp.where(parity == 1, from_a[p // 2], from_b[p // 2])[:, at]
                right = jnp.where(parity == 1, from_b[p // 2], from_a[p // 2])[:, at]
                ext[p, HALO : HALO + core, :] = jnp.concatenate([left, tile[p], right], axis=1)
        planes, k = win.shape[0], win.shape[1]
        q = z % step_rows
        row, col = spot(pos, q)
        for p in range(planes):
            win[p] = window(ext.at[p], row, col, k)
        owned[...] = ext[z]
        half = probes.shape[0] // step_rows
        part[...] = forward_modes(win, probes, cos_t, sin_t, table, u_out, psi_out, 0, half)

    return body


def more_forward(win, probe, cos_t, sin_t, table, before, p_in, u_in, psi_in, part, probes, u_out, psi_out):
    first, last = probes.shape[0] - probe.shape[0], probes.shape[0]
    probes[first:last] = probe[...]
    part[...] = before[...] + forward_modes(
        win, probes, cos_t, sin_t, table, u_out, psi_out, first, last
    )


def next_forward(group, count):
    def body(index, *refs):
        pieces, refs = refs[:count], refs[count:]
        probes, cos_t, sin_t, table, win, part, u_out, psi_out = refs
        z = place(index, group)[0]
        for j, piece in enumerate(pieces):
            win[z ^ j] = piece[...]
        part[...] = forward_modes(
            win, probes, cos_t, sin_t, table, u_out, psi_out, 0, probes.shape[0]
        )

    return body


def backward(step, step_rows, group, parts, count):
    def body(index, *refs):
        partials, refs = refs[:parts], refs[parts:]
        measured, win, probes, u_in, psi_in, cos_t, sin_t, table = refs[:8]
        sends, grads = refs[8 : 8 + count], refs[8 + count]
        z = place(index, group)[0]
        k = win.shape[1]
        high, low = table[0], table[1]
        cos, sin = cos_t[...], sin_t[...]
        total = partials[0][...]
        for extra in partials[1:]:
            total = total + extra[...]
        sends[1][1] = total
        twice = (2.0 * (total - measured[step * step_rows + z % step_rows])).T
        br, bi = 1.0 + win[2], win[3]
        zero = jnp.zeros((k, k), f32)
        waves = []
        for m in range(probes.shape[0]):
            psi = psi_in[m]
            waves.append(pair(twice * psi[:, :k], -(twice * psi[:, k:])))
        turned = []
        sum_r, sum_i = zero, zero
        for m, g in enumerate(dft(waves, high, low)):
            gr, gi = g[:, :k], -g[:, k:]
            u = u_in[m]
            ur, ui = u[:, :k], u[:, k:]
            sum_r = sum_r + (ur * gr - ui * gi)
            sum_i = sum_i + (ur * gi + ui * gr)
            turned.append(pair(br * gr + bi * gi, br * gi - bi * gr))
        grads[2], grads[3] = sum_r, sum_i
        waves = []
        for s in dft(turned, high, low):
            sr, si = s[:, :k], s[:, k:]
            waves.append(pair(cos * sr + sin * si, sin * sr - cos * si))
        sum_r, sum_i = zero, zero
        for m, g in enumerate(dft(waves, high, low)):
            gr, gi = g[:, :k], -g[:, k:]
            pr, pi = probes[m, 0], probes[m, 1]
            sum_r = sum_r + (pr * gr + pi * gi)
            sum_i = sum_i + (pr * gi - pi * gr)
        grads[0], grads[1] = sum_r, sum_i
        for j in range(count):
            if j == 1:
                sends[j][0] = grads[z ^ j]
            else:
                sends[j][...] = grads[z ^ j]

    return body


def sides(parity, left, right):
    return jnp.where(parity == 1, left, right), jnp.where(parity == 1, right, left)


def scatter(step, step_rows, group, count, rows):
    def body(index, pos, *refs):
        pieces, outs, ext = refs[:count], refs[count:-1], refs[-1]
        z, parity = place(index, group)
        q = z % step_rows
        width = ext.shape[1]
        ext[...] = jnp.zeros(ext.shape, f32)
        values = [piece[0] if j == 1 else piece[...] for j, piece in enumerate(pieces)]
        for i in range(step_rows):
            total = values[i]
            for j in range(i + step_rows, count, step_rows):
                total = total + values[j]
            which = step * step_rows + (q ^ i)
            add_window(ext, total, *spot(pos, which))
        if rows:
            outs[0][...] = ext[...]
        else:
            half = width // 2
            core = outs[0].shape[0]
            middle = ext[HALO : HALO + core, :]
            outs[0][...], outs[1][...] = sides(parity, middle[:, :half], middle[:, half:])

    return body


def updated_rows(parity, out_a, out_b, from_a, from_b, owned):
    left, right = sides(parity, out_a[...] + from_a[...], out_b[...] + from_b[...])
    grad = pair(left, right)
    return owned[HALO : HALO + grad.shape[0], :] - learning_rate * grad


def next_windows(step, step_rows, source, z, pos, outs):
    q = z % step_rows
    k = outs[0].shape[0]
    for i, out in enumerate(outs):
        which = step * step_rows + (q ^ i)
        out[...] = window(source, *spot(pos, which), k)


def update(step, step_rows, group):
    def body(index, pos, out_a, out_b, from_a, from_b, owned, fresh, *outs):
        z, parity = place(index, group)
        fresh[...] = jnp.zeros(fresh.shape, f32)
        fresh[HALO : HALO + out_a.shape[0], :] = updated_rows(parity, out_a, out_b, from_a, from_b, owned)
        next_windows(step, step_rows, fresh, z, pos, outs)

    return body


def update_middle(group):
    def body(index, out_a, out_b, from_a, from_b, owned, middle):
        middle[...] = updated_rows(place(index, group)[1], out_a, out_b, from_a, from_b, owned)

    return body


def only_windows(step, step_rows, group):
    def body(index, pos, owned, *outs):
        next_windows(step, step_rows, owned, place(index, group)[0], pos, outs)

    return body


def last_update(group):
    def body(index, out_a, out_b, from_a, from_b, owned, core):
        middle = updated_rows(place(index, group)[1], out_a, out_b, from_a, from_b, owned)
        core[...] = middle[:, HALO : middle.shape[1] - HALO]

    return body


def gather_planes(group, count):
    def body(index, *refs):
        out = refs[count]
        for j in range(count):
            out[place(index, group)[0] ^ j] = refs[j][...]

    return body


def gather_intensities(step_rows, group):
    def body(index, *refs):
        out = refs[-1]
        q = place(index, group)[0] % step_rows
        for i, ref in enumerate(refs[:-1]):
            step, j = divmod(i, step_rows)
            out[step * step_rows + (q ^ j)] = ref[1]

    return body


def across(value, axis, bits):
    return lax.ppermute(value, axis, [(i, i ^ bits) for i in range(lax.axis_size(axis))])


def in_pair(value):
    return across(value, "tile", 1)


def between_pairs(value):
    count = lax.axis_size("tile")
    return lax.ppermute(value, "tile", [(i, (i + (1 if i % 2 else -1)) % count) for i in range(count)])


def from_behind(value, axis, steps):
    count = lax.axis_size(axis)
    first, last = (max(0, -steps), min(count, count - steps))
    return lax.ppermute(value, axis, [(source, source + steps) for source in range(first, last)])


def local(object_tiles, probe, propagator_phase, measured, positions):
    layers, core = object_tiles.shape[1], object_tiles.shape[3]
    count = layers * 2
    k = probe.shape[-1]
    step_rows = positions.shape[0] // STEPS
    modes = probe.shape[0] * step_rows
    group, tiles = lax.axis_size("mode"), lax.axis_size("tile")
    assert layers == 2 and count == group and step_rows == 2 and core == 2 * HALO
    assert tiles % 2 == 0 and tiles > 2
    rows = tiles > TILE_COLS
    extent = core + 2 * HALO
    tall = (extent + SUB, extent)
    tile = lax.axis_index("tile")
    index = (tile * group + lax.axis_index("mode")).astype(jnp.int32).reshape(1)
    planes = object_tiles.reshape(count, core, core)
    flat, wave, held = (k, k), (modes, k, 2 * k), (modes,) + probe.shape[1:]

    other_probe = across(probe, "mode", 1)
    packed = (count // 2, core, 2 * HALO)
    out_a, out_b, planes = call(pack(group), [packed, packed, planes.shape], (index, planes))
    from_a, from_b = in_pair(out_a), between_pairs(out_b)
    cos_t, sin_t = jnp.cos(propagator_phase.T), jnp.sin(propagator_phase.T)
    optics = (cos_t, sin_t, jnp.asarray(dft_matrix(k)))
    (probes,) = call(hold, [held], (probe,))

    if rows:

        def unpacked(value):
            return value.reshape(-1, core, 2, HALO).transpose(0, 2, 1, 3).reshape(count, core, HALO)

        left, right = sides(tile % 2, from_a, from_b)
        wide = jnp.concatenate([unpacked(left), planes, unpacked(right)], axis=2)
        above = from_behind(wide[:, core - HALO :], "tile", TILE_COLS)
        below = from_behind(wide[:, :HALO], "tile", -TILE_COLS)
        slack = jnp.zeros((count, SUB, extent), f32)
        objects = (jnp.concatenate([above, wide, below, slack], axis=1),)
    else:
        objects = (planes, from_a, from_b)

    win, owned, part, u, psi = call(
        first_forward(step_rows, group, rows),
        [(count, k, k), tall, flat, wave, wave],
        (index, positions) + objects + (probes,) + optics,
        [pltpu.VMEM((count,) + tall, f32)],
    )
    part, probes, u, psi = call(
        more_forward,
        [flat, held, wave, wave],
        (win, other_probe) + optics + (part, probes, u, psi),
        aliases={6: 1, 7: 2, 8: 3},
    )

    kept = []
    for step in range(STEPS):
        partials = [part] + [across(part, "mode", j) for j in range(step_rows, group, step_rows)]
        sends = call(
            backward(step, step_rows, group, len(partials), count),
            [flat, (2,) + flat] + [flat] * (count - 2),
            (index,) + tuple(partials) + (measured, win, probes, u, psi) + optics,
            [pltpu.VMEM((count, k, k), f32)],
        )
        pieces = [sends[0]] + [across(sends[j], "mode", j) for j in range(1, group)]
        kept += [sends[1], pieces[1]]
        half = (core, extent // 2)
        grads = call(
            scatter(step, step_rows, group, count, rows),
            [tall] if rows else [half, half],
            (index, positions) + tuple(pieces),
            [pltpu.VMEM(tall, f32)],
        )
        if rows:
            whole = grads[0]
            middle = whole[HALO : HALO + core]
            middle = middle.at[core - HALO :].add(from_behind(whole[:HALO], "tile", -TILE_COLS))
            middle = middle.at[:HALO].add(from_behind(whole[HALO + core : extent], "tile", TILE_COLS))
            grads = sides(tile % 2, middle[:, : extent // 2], middle[:, extent // 2 :])
        out_a, out_b = grads
        from_a = in_pair(out_a)
        from_b = between_pairs(out_b)
        sums = (out_a, out_b, from_a, from_b, owned)
        if step + 1 == STEPS:
            break
        if rows:
            (middle,) = call(update_middle(group), [(core, extent)], (index,) + sums)
            above = from_behind(middle[core - HALO :], "tile", TILE_COLS)
            below = from_behind(middle[:HALO], "tile", -TILE_COLS)
            slack = jnp.zeros((SUB, extent), f32)
            owned = jnp.concatenate([above, middle, below, slack], axis=0)
            outs = call(only_windows(step + 1, step_rows, group), [flat] * step_rows, (index, positions, owned))
        else:
            out = call(
                update(step + 1, step_rows, group),
                [tall] + [flat] * step_rows,
                (index, positions) + sums,
            )
            owned, outs = out[0], out[1:]
        pieces = [outs[0]] + [across(outs[j % step_rows], "mode", j) for j in range(1, group)]
        win, part, u, psi = call(
            next_forward(group, count),
            [(count, k, k), flat, wave, wave],
            (index,) + tuple(pieces) + (probes,) + optics,
        )

    (plane,) = call(last_update(group), [(core, core)], (index,) + sums)
    pieces = [plane]
    for j in range(1, group):
        pieces.append(across(plane, "mode", j))
    (updated,) = call(gather_planes(group, count), [(count, core, core)], (index,) + tuple(pieces))
    (intensities,) = call(gather_intensities(step_rows, group), [measured.shape], (index,) + tuple(kept))
    return (updated.reshape(object_tiles.shape), intensities)


def solution(mesh):
    return jax.shard_map(
        local,
        mesh=mesh,
        in_specs=(
            P("tile", None, None, None, None),
            P("mode", None, None, None),
            P(),
            P("tile", None, None),
            P("tile", None),
        ),
        out_specs=(P("tile", None, None, None, None), P("tile", None, None)),
        check_vma=False,
    )
```
